32 devices in a mesh: row: 8 (over z, y), col: 4 (over x, core).
Axes of the slice: x: 2, y: 2, z: 4, core: 2. Of those that a mesh axis runs over, the one named last changes fastest.
Arguments:
- features: bfloat16 [6144, 4096], P(('row', 'col')), may hold values from -6 to 6
- cotangent: bfloat16 [6144, 8192], P(('row', 'col')), may hold values from -0.078125 to 0.078125
Outputs:
- weight_grad: float32 [4096, 8192], P('row', 'col')
The draws below stay inside these ranges and needn't reach their ends.
All inputs are finite; a program needn't handle non-finite values.
Results may differ from the reference program's by a relative error of at most 0.0003.
Values may be sent and summed in bfloat16 or wider, within the bound.
A program may use at most 256 MiB of HBM per device.

```python
import jax
import jax.numpy as jnp
from jax import lax

DIN = 4096
DOUT = 8192
TOK_DEV = 192
TOKENS = 6144
N_ROW = 8
N_COL = 4


def strengthened(array, rng, source, target, blocks, factor):
    owner, partner = [(jnp.arange(array.shape[position]) // (array.shape[position] // blocks)).reshape([-1 if axis == position else 1 for axis in range(array.ndim)]) for position in (source, target)]
    chosen = jax.random.permutation(rng, blocks)[partner]
    strong = (owner == chosen) | (owner == (partner + blocks // 2) % blocks)
    return jnp.where(strong, factor * array, array)


def block_levels(own_key, extent, split, low, high):
    def one(position, shards_of):
        heights = jax.random.uniform(jax.random.fold_in(jax.random.fold_in(own_key, 6), position), (shards_of,), jnp.float32, low / len(split), high / len(split))
        return jnp.repeat(jnp.exp(heights), extent[position] // shards_of).reshape((-1,) + (1,) * (len(extent) - position - 1))

    level = one(*split[0])
    for cut in split[1:]:
        level = level * one(*cut)
    return level


def centred(stream_key, shape, width, most, cuts=(), dtype=jnp.bfloat16):
    values = jax.random.normal(stream_key, shape, jnp.float32) * width
    if len(cuts) > 0:
        values = block_levels(stream_key, shape, cuts, -0.22, 0.18) * values
    return jnp.clip(values, min=-most, max=most).astype(dtype)


def heavy_noise(key, shape, deviation, bound, shards, heavy, kind=jnp.bfloat16):
    drawn = deviation * jax.random.normal(key, shape, jnp.float32)
    if shards:
        drawn = drawn * block_levels(key, shape, shards, -0.22, 0.18)
    return jnp.clip(strengthened(drawn, jax.random.fold_in(key, 3), *heavy), -bound, bound).astype(kind)


def setup_inputs(seed: int = 0) -> dict:
    key_of = jax.random.split(jax.random.key(seed), 3)
    features = heavy_noise(key_of[0], (TOKENS, DIN), 1.0, 6.0, ((0, 32),), (0, 1, 32, 2.75))
    cotangent = centred(key_of[1], (TOKENS, DOUT), TOKENS ** -0.5, 0.078125, ((0, 32),))
    return {"features": features, "cotangent": cotangent}


def reference(features, cotangent):
    block_rows = TOK_DEV * N_COL
    feature_blocks = features.reshape(N_ROW, block_rows, DIN)
    cotangent_blocks = cotangent.reshape(N_ROW, block_rows, DOUT)

    def accumulate(running, paired):
        left = paired[0].astype(jnp.float32)
        right = paired[1].astype(jnp.float32)
        return running + jnp.dot(left.T, right, precision=lax.Precision.HIGHEST), None

    initial = jnp.zeros((DIN, DOUT), jnp.float32)
    weight_grad, unused = lax.scan(accumulate, initial, (feature_blocks, cotangent_blocks))
    return weight_grad
```

```python
import functools

import jax
import jax.numpy as jnp
from jax import lax
from jax.experimental import pallas as pl
from jax.experimental.pallas import tpu as pltpu
from jax.sharding import PartitionSpec as P

MESH = pl.DeviceIdType.MESH
CHUNK = 512
STRIP = 32
PAD = 16
PEAK = 181.0
VMEM_MOST = 60 * 1024 * 1024


def tokens_product(left, right):
    return lax.dot_general(
        left, right, (((0,), (0,)), ((), ())), preferred_element_type=jnp.float32
    )


def plain(features, cotangent):
    row_count = lax.axis_size("row")
    width_in = features.shape[1]
    local_rows = width_in // row_count
    columns = lax.all_to_all(cotangent, "col", split_axis=1, concat_axis=0, tiled=True)
    tok_local = features.shape[0]
    exchanged = lax.all_to_all(features, "row", split_axis=1, concat_axis=0, tiled=True)
    stacked = exchanged.reshape(row_count, tok_local, local_rows)
    gathered = lax.all_gather(stacked, "col", axis=1, tiled=True)
    all_tokens = gathered.reshape(-1, local_rows)
    return tokens_product(all_tokens, lax.all_gather(columns, "row", axis=0, tiled=True))


def encode(src, dst):
    rows, width = src.shape

    def strip(s):
        return pl.ds(pl.multiple_of(s * STRIP, STRIP), STRIP)

    top = lax.fori_loop(
        0, rows // STRIP, lambda s, m: jnp.maximum(m, jnp.abs(src[strip(s), :])),
        jnp.zeros((STRIP, width), jnp.float32),
    )
    top = jnp.max(top, axis=0, keepdims=True)
    undo = (jnp.maximum(top, 1e-30) * (1.0 / PEAK)).astype(jnp.bfloat16)
    dst[pl.ds(rows, PAD), :] = jnp.broadcast_to(undo, (PAD, width))
    scale = 1.0 / undo.astype(jnp.float32)

    @pl.loop(0, rows // STRIP)
    def _(s):
        t = src[strip(s), :] * scale
        u = t * t
        u = u * u
        u = u * u
        u = u * u
        dst[strip(s), :] = jnp.where(t < 0, -u, u).astype(jnp.bfloat16)


def decode_add(src, into):
    rows = into.shape[0]
    undo = src[pl.ds(rows, PAD), :].astype(jnp.float32)[:1]

    @pl.loop(0, rows // STRIP)
    def _(s):
        span = pl.ds(pl.multiple_of(s * STRIP, STRIP), STRIP)
        b = src[span, :].astype(jnp.float32)
        root = lax.rsqrt(jnp.maximum(jnp.abs(b), 1e-37))
        most = lax.rsqrt(lax.rsqrt(lax.rsqrt(root)))
        into[span, :] += (b * root) * root * most * undo


def kernel(
    lines, cols, feat, cot, out,
    fall, dall, tmp, ysend, yrecv, acc, msend, mrecv,
    fl, fz_s, fz_r, fx_s, fx_r, fm_s, fm_r,
    dl, dx_s, dx_r, dz_s, dz_r, y_s, y_r, m_s, m_r, o_s,
):
    row = lax.axis_index("row")
    col = lax.axis_index("col")
    z, y = row // 2, row % 2
    here = z % 2
    near = z + 1 - 2 * here
    far = lines - 1 - z
    tok = feat.shape[0]
    rows = fall.shape[2]
    half = rows // 2
    chunks = dall.shape[0]
    width = chunks * CHUNK

    def at_row(zz, yy):
        return {"row": zz * 2 + yy, "col": col}

    def at_col(d):
        return {"row": row, "col": (col + d) % cols}

    pair, mirror, partner = at_row(near, y), at_row(far, y), at_row(z, 1 - y)
    across = 2
    mate_col = col + 1 - 2 * (col % 2)
    mate = {"row": row, "col": mate_col}

    def remote(src, dst, s, r, dev):
        return pltpu.make_async_remote_copy(
            src_ref=src, dst_ref=dst, send_sem=s, recv_sem=r,
            device_id=dev, device_id_type=MESH,
        )

    barrier = pltpu.get_barrier_semaphore()
    others = [pair, mirror, partner] + [at_col(d) for d in range(1, cols)]
    for dev in others:
        pl.semaphore_signal(barrier, inc=1, device_id=dev, device_id_type=MESH)
    pl.semaphore_wait(barrier, len(others))

    def slot(plane, c):
        return pl.ds(pl.multiple_of((plane * cols + c) * tok, tok), tok)

    def f_cols(zz):
        return feat.at[:, pl.ds(pl.multiple_of(zz * rows, rows), rows)]

    def wanted(zz, g):
        return lines - 1 - zz if g == 0 else zz

    def f_own(g):
        return pltpu.make_async_copy(f_cols(wanted(z, g)), fall.at[g, slot(here, col)], fl.at[g])

    def f_pair(g):
        return remote(
            f_cols(wanted(near, g)), fall.at[g, slot(here, col)], fz_s.at[g], fz_r.at[g], pair
        )

    def f_block(g, other, c):
        return fall.at[g, slot(1 - here if other else here, c)]

    def f_across(g, other):
        block = f_block(g, other, col)
        src = block if other else f_cols(wanted(z, g))
        return remote(src, block, fx_s.at[g, other], fx_r.at[g, other], at_col(across))

    def f_mate(g, other, k):
        block = f_block(g, other, (col + across * k) % cols)
        src = f_cols(wanted(z, g)) if not other and not k else block
        return remote(src, block, fm_s.at[g, other, k], fm_r.at[g, other, k], mate)

    def d_cols(cc, j):
        return cot.at[:, pl.ds(pl.multiple_of(cc * width + j * CHUNK, CHUNK), CHUNK)]

    def d_own(j):
        return pltpu.make_async_copy(d_cols(col, j), dall.at[j, slot(here, col)], dl.at[j])

    def d_send(j, d):
        return remote(
            d_cols((col + d) % cols, j), dall.at[j, slot(here, col)],
            dx_s.at[j, d], dx_r.at[j, d], at_col(d),
        )

    def d_pair(j, d):
        block = dall.at[j, slot(here, (col + cols - d) % cols)]
        return remote(
            d_cols(col, j) if d == 0 else block, block, dz_s.at[j, d], dz_r.at[j, d], pair
        )

    def y_copy(g, j):
        return remote(ysend.at[g, j], yrecv.at[g, j], y_s.at[g, j], y_r.at[g, j], partner)

    def m_copy(j):
        return remote(msend.at[j], mrecv.at[j], m_s.at[j], m_r.at[j], mirror)

    def out_copy(j):
        return pltpu.make_async_copy(acc.at[1, j], out.at[:, pl.ds(j * CHUNK, CHUNK)], o_s.at[j])

    def d_issue(j):
        d_own(j).start()
        d_pair(j, 0).start()
        for d in (1, 3, 2):
            d_send(j, d).start()

    def d_relay(j):
        for d in (1, 3, 2):
            d_send(j, d).wait_recv()
            d_pair(j, d).start()

    def f_issue(g):
        f_pair(g).start()
        f_across(g, 0).start()
        f_mate(g, 0, 0).start()
        f_own(g).start()

    def f_relay(g):
        f_across(g, 0).wait_recv()
        f_mate(g, 0, 1).start()
        f_pair(g).wait_recv()
        f_across(g, 1).start()
        f_mate(g, 1, 0).start()

    def f_end(g):
        f_across(g, 1).wait_recv()
        f_mate(g, 1, 1).start()
        f_own(g).wait()
        for other in range(2):
            for k in range(2):
                f_mate(g, other, k).wait_recv()

    def d_end(j):
        d_own(j).wait()
        for d in range(cols):
            d_pair(j, d).wait_recv()

    def columns_of(which):
        return pl.ds(pl.multiple_of(which * half, half), half)

    def multiply(g, j):
        tmp[...] = tokens_product(fall[g, :, columns_of(1 - y)], dall[j])
        encode(tmp, ysend.at[g, j])
        y_copy(g, j).start()
        acc[g, j] = tokens_product(fall[g, :, columns_of(y)], dall[j])

    def finish(g, j):
        y_copy(g, j).wait_recv()
        decode_add(yrecv.at[g, j], acc.at[g, j])
        if g == 0:
            encode(acc.at[0, j], msend.at[j])
            m_copy(j).start()

    f_issue(0)
    d_issue(0)
    f_relay(0)
    d_relay(0)
    f_issue(1)
    d_issue(1)
    f_end(0)
    for i in range(chunks):
        if i + 1 < chunks:
            d_relay(i + 1)
        if i + 2 < chunks:
            d_issue(i + 2)
        d_end(i)
        multiply(0, i)
        if i == 0:
            f_relay(1)
            f_end(1)
        multiply(1, i)
        if i >= 1:
            finish(1, i - 1)
        finish(0, i)
    finish(1, chunks - 1)
    for j in range(chunks):
        m_copy(j).wait_recv()
        decode_add(mrecv.at[j], acc.at[1, j])
        out_copy(j).start()

    for g in range(2):
        f_pair(g).wait_send()
        for other in range(2):
            f_across(g, other).wait_send()
            for k in range(2):
                f_mate(g, other, k).wait_send()
    for j in range(chunks):
        for d in range(cols):
            d_pair(j, d).wait_send()
        for d in range(1, cols):
            d_send(j, d).wait_send()
        for g in range(2):
            y_copy(g, j).wait_send()
        m_copy(j).wait_send()
        out_copy(j).wait()


def sizes(row_count, cols, features, cotangent):
    lines = row_count // 2
    tokens = 2 * features.shape[0] * cols
    rows = features.shape[1] // lines
    width = cotangent.shape[1] // cols
    return lines, tokens, rows, width


def fused(row_count, cols, features, cotangent):
    lines, tokens, rows, width = sizes(row_count, cols, features, cotangent)
    chunks = width // CHUNK
    half = rows // 2
    dma = pltpu.SemaphoreType.DMA
    coded = pltpu.VMEM((2, chunks, half + PAD, CHUNK), jnp.bfloat16)
    moved = pltpu.VMEM((chunks, half + PAD, CHUNK), jnp.bfloat16)
    return pl.pallas_call(
        functools.partial(kernel, lines, cols),
        out_shape=jax.ShapeDtypeStruct((half, width), jnp.float32),
        in_specs=[pl.BlockSpec(memory_space=pl.ANY)] * 2,
        out_specs=pl.BlockSpec(memory_space=pl.ANY),
        scratch_shapes=[
            pltpu.VMEM((2, tokens, rows), jnp.bfloat16),
            pltpu.VMEM((chunks, tokens, CHUNK), jnp.bfloat16),
            pltpu.VMEM((half, CHUNK), jnp.float32),
            coded, coded,
            pltpu.VMEM((2, chunks, half, CHUNK), jnp.float32),
            moved, moved,
            dma((2,)), dma((2,)), dma((2,)),
            dma((2, 2)), dma((2, 2)), dma((2, 2, 2)), dma((2, 2, 2)),
            dma((chunks,)), dma((chunks, cols)), dma((chunks, cols)),
            dma((chunks, cols)), dma((chunks, cols)),
            dma((2, chunks)), dma((2, chunks)), dma((chunks,)), dma((chunks,)),
            dma((chunks,)),
        ],
        compiler_params=pltpu.CompilerParams(
            collective_id=0, has_side_effects=True, vmem_limit_bytes=VMEM_MOST
        ),
    )(features, cotangent)


def fits(row_count, cols, features, cotangent):
    if row_count != 8 or cols != 4 or cotangent.shape[1] % (cols * CHUNK):
        return False
    if features.shape[1] % (row_count * 128) or features.shape[0] % 16:
        return False
    lines, tokens, rows, width = sizes(row_count, cols, features, cotangent)
    held = 2 * tokens * (2 * rows + width) + 11 * rows * width + 4 * rows * CHUNK
    return held <= VMEM_MOST


def local(row_count, cols, features, cotangent):
    if fits(row_count, cols, features, cotangent):
        return fused(row_count, cols, features, cotangent)
    return plain(features, cotangent)


def solution(mesh):
    placed = (P(("row", "col"), None), P(("row", "col"), None))
    body = functools.partial(local, mesh.shape["row"], mesh.shape["col"])
    return jax.shard_map(
        body, mesh=mesh, in_specs=placed, out_specs=P("row", "col"), check_vma=False
    )
```

```python
import functools

import jax
import jax.numpy as jnp
from jax import lax
from jax.experimental import pallas as pl
from jax.experimental.pallas import tpu as pltpu
from jax.sharding import PartitionSpec as P

MESH = pl.DeviceIdType.MESH
CHUNKS = 8
STRIP = 32
PAD = 16
PEAK = 181.0
VMEM_MOST = 60 * 1024 * 1024


ORDER = (
    ("F", 0), ("D", 0), ("F", 2), ("relay", 0), ("D", 1), ("forward", "F", 0), ("relay", 1),
    ("D", 2), ("relay_across", 0), ("relay", 2), ("D", 3), ("forward", "F", 2), ("relay", 3),
    ("P", 0), ("relay_across", 1), ("D", 4), ("relay_across", 2), ("relay", 4), ("D", 5),
    ("relay_across", 3), ("relay", 5), ("D", 6), ("forward", "P", 0), ("give", 0, 0),
    ("relay", 6), ("P", 2), ("relay_across", 4), ("give", 0, 1), ("D", 7), ("relay_across", 5),
    ("relay", 7), ("give", 0, 2), ("F", 1), ("relay_across", 6), ("F", 3), ("forward", "P", 2),
    ("keep", 0, 0), ("finish", 0, 0), ("give", 0, 3), ("relay_across", 7), ("keep", 0, 1),
    ("finish", 0, 1), ("keep", 0, 2), ("finish", 0, 2), ("forward", "F", 1), ("keep", 0, 3),
    ("finish", 0, 3), ("forward", "F", 3), ("give", 0, 4), ("keep", 0, 4), ("give", 0, 5),
    ("keep", 0, 5), ("finish", 0, 4), ("P", 1), ("finish", 0, 5), ("give", 0, 6), ("keep", 0, 6),
    ("forward", "P", 1), ("give", 1, 0), ("P", 3), ("give", 1, 1), ("give", 1, 2),
    ("give", 1, 3), ("finish", 0, 6), ("give", 1, 4), ("forward", "P", 3), ("give", 1, 5),
    ("keep", 1, 0), ("keep", 1, 1), ("keep", 1, 2), ("keep", 1, 3), ("keep", 1, 4),
    ("keep", 1, 5), ("keep", 1, 6), ("give", 0, 7), ("keep", 0, 7), ("keep", 1, 7),
    ("finish", 1, 0), ("finish", 1, 1), ("give", 1, 6), ("finish", 1, 2), ("give", 1, 7),
    ("last", 0), ("last", 1), ("finish", 1, 3), ("last", 2), ("finish", 1, 4), ("last", 3),
    ("finish", 1, 5), ("last", 4), ("finish", 0, 7), ("last", 5), ("finish", 1, 6),
    ("finish", 1, 7), ("last", 6), ("last", 7),
)


def tokens_product(left, right):
    return lax.dot_general(
        left, right, (((0,), (0,)), ((), ())), preferred_element_type=jnp.float32
    )


def plain(features, cotangent):
    row_count = lax.axis_size("row")
    width_in = features.shape[1]
    local_rows = width_in // row_count
    columns = lax.all_to_all(cotangent, "col", split_axis=1, concat_axis=0, tiled=True)
    tok_local = features.shape[0]
    exchanged = lax.all_to_all(features, "row", split_axis=1, concat_axis=0, tiled=True)
    stacked = exchanged.reshape(row_count, tok_local, local_rows)
    gathered = lax.all_gather(stacked, "col", axis=1, tiled=True)
    all_tokens = gathered.reshape(-1, local_rows)
    return tokens_product(all_tokens, lax.all_gather(columns, "row", axis=0, tiled=True))


def encode(src, dst):
    rows, width = src.shape

    def strip(s):
        return pl.ds(pl.multiple_of(s * STRIP, STRIP), STRIP)

    top = lax.fori_loop(
        0, rows // STRIP, lambda s, m: jnp.maximum(m, jnp.abs(src[strip(s), :])),
        jnp.zeros((STRIP, width), jnp.float32),
    )
    top = jnp.max(top, axis=0, keepdims=True)
    undo = (jnp.maximum(top, 1e-30) * (1.0 / PEAK)).astype(jnp.bfloat16)
    dst[pl.ds(rows, PAD), :] = jnp.broadcast_to(undo, (PAD, width))
    scale = 1.0 / undo.astype(jnp.float32)

    @pl.loop(0, rows // STRIP)
    def _(s):
        t = src[strip(s), :] * scale
        u = t * t
        u = u * u
        u = u * u
        u = u * u
        dst[strip(s), :] = jnp.where(t < 0, -u, u).astype(jnp.bfloat16)


def decode_add(src, into):
    rows = into.shape[0]
    undo = src[pl.ds(rows, PAD), :].astype(jnp.float32)[:1]

    @pl.loop(0, rows // STRIP)
    def _(s):
        span = pl.ds(pl.multiple_of(s * STRIP, STRIP), STRIP)
        b = src[span, :].astype(jnp.float32)
        root = lax.rsqrt(jnp.maximum(jnp.abs(b), 1e-37))
        most = lax.rsqrt(lax.rsqrt(lax.rsqrt(root)))
        into[span, :] += (b * root) * root * most * undo


def kernel(
    lines, cols, feat, cot, out,
    fall, dall, tmp, ysend, yrecv, acc, msend, mrecv,
    fl, fz_s, fz_r, fx_s, fx_r, fm_s, fm_r,
    dl, dx_s, dx_r, dz_s, dz_r, y_s, y_r, m_s, m_r, o_s,
):
    row = lax.axis_index("row")
    col = lax.axis_index("col")
    z, y = row // 2, row % 2
    here = z % 2
    near = z + 1 - 2 * here
    far = lines - 1 - z
    tok = feat.shape[0]
    half = fall.shape[2]
    chunks, _, chunk = dall.shape
    width = chunks * chunk

    def at_row(zz, yy):
        return {"row": zz * 2 + yy, "col": col}

    pair, mirror, partner = at_row(near, y), at_row(far, y), at_row(z, 1 - y)
    mate_col = col + 1 - 2 * (col % 2)
    col_of = (col, mate_col, (col + 2) % cols, (mate_col + 2) % cols)
    MATE, ACROSS = 1, 2

    def at_col(k):
        return {"row": row, "col": col_of[k]}

    def remote(src, dst, s, r, dev):
        return pltpu.make_async_remote_copy(
            src_ref=src, dst_ref=dst, send_sem=s, recv_sem=r,
            device_id=dev, device_id_type=MESH,
        )

    barrier = pltpu.get_barrier_semaphore()
    others = [pair, mirror, partner] + [at_col(k) for k in range(1, cols)]
    for dev in others:
        pl.semaphore_signal(barrier, inc=1, device_id=dev, device_id_type=MESH)
    pl.semaphore_wait(barrier, len(others))

    def slot(plane, c):
        return pl.ds(pl.multiple_of((plane * cols + c) * tok, tok), tok)

    def f_cols(zz, q):
        wanted = lines - 1 - zz if q % 2 == 0 else zz
        yy = 1 - y if q < 2 else y
        return feat.at[:, pl.ds(pl.multiple_of((wanted * 2 + yy) * half, half), half)]

    def f_own(q):
        return pltpu.make_async_copy(f_cols(z, q), fall.at[q, slot(here, col)], fl.at[q])

    def f_pair(q):
        return remote(f_cols(near, q), fall.at[q, slot(here, col)], fz_s.at[q], fz_r.at[q], pair)

    def f_block(q, other, k):
        return fall.at[q, slot(1 - here if other else here, col_of[k])]

    def f_across(q, other):
        block = f_block(q, other, 0)
        src = block if other else f_cols(z, q)
        return remote(src, block, fx_s.at[q, other], fx_r.at[q, other], at_col(ACROSS))

    def f_mate(q, other, k):
        block = f_block(q, other, ACROSS * k)
        src = f_cols(z, q) if not other and not k else block
        return remote(src, block, fm_s.at[q, other, k], fm_r.at[q, other, k], at_col(MATE))

    def d_cols(cc, j):
        return cot.at[:, pl.ds(pl.multiple_of(cc * width + j * chunk, chunk), chunk)]

    def d_own(j):
        return pltpu.make_async_copy(d_cols(col, j), dall.at[j, slot(here, col)], dl.at[j])

    def d_send(j, k):
        return remote(
            d_cols(col_of[k], j), dall.at[j, slot(here, col)],
            dx_s.at[j, k], dx_r.at[j, k], at_col(k),
        )

    def d_pair(j, k):
        block = dall.at[j, slot(here, col_of[k])]
        return remote(
            block if k else d_cols(col, j), block, dz_s.at[j, k], dz_r.at[j, k], pair
        )

    def y_copy(g, j):
        return remote(ysend.at[g, j], yrecv.at[g, j], y_s.at[g, j], y_r.at[g, j], partner)

    def m_copy(j):
        return remote(msend.at[j], mrecv.at[j], m_s.at[j], m_r.at[j], mirror)

    def out_copy(j):
        return pltpu.make_async_copy(acc.at[1, j], out.at[:, pl.ds(j * chunk, chunk)], o_s.at[j])

    ready = set()

    def once(key):
        new = key not in ready
        ready.add(key)
        return new

    def arrive(q, j):
        if once(("F", q)):
            f_own(q).wait()
            for other in range(2):
                for k in range(2):
                    f_mate(q, other, k).wait_recv()
        if once(("D", j)):
            d_own(j).wait()
            for k in range(cols):
                d_pair(j, k).wait_recv()

    def do_F(q):
        f_pair(q).start()
        f_across(q, 0).start()
        f_mate(q, 0, 0).start()
        f_own(q).start()

    def do_P(q):
        f_pair(q).wait_recv()
        f_across(q, 1).start()
        f_mate(q, 1, 0).start()

    def do_D(j):
        d_pair(j, 0).start()
        for k in (2, 3, 1):
            d_send(j, k).start()
        d_own(j).start()

    def do_forward(kind, q):
        other = 1 if kind == "P" else 0
        f_across(q, other).wait_recv()
        f_mate(q, other, 1).start()

    def do_relay(j):
        d_send(j, MATE).wait_recv()
        d_pair(j, MATE).start()

    def do_relay_across(j):
        for k in (2, 3):
            d_send(j, k).wait_recv()
            d_pair(j, k).start()

    def do_give(g, j):
        arrive(g, j)
        tmp[...] = tokens_product(fall[g], dall[j])
        encode(tmp, ysend.at[g, j])
        y_copy(g, j).start()

    def do_keep(g, j):
        arrive(2 + g, j)
        acc[g, j] = tokens_product(fall[2 + g], dall[j])

    def do_finish(g, j):
        y_copy(g, j).wait_recv()
        decode_add(yrecv.at[g, j], acc.at[g, j])
        if g == 0:
            encode(acc.at[0, j], msend.at[j])
            m_copy(j).start()

    def do_last(j):
        m_copy(j).wait_recv()
        decode_add(mrecv.at[j], acc.at[1, j])
        out_copy(j).start()

    run = {
        "F": do_F, "P": do_P, "D": do_D, "forward": do_forward, "relay": do_relay,
        "relay_across": do_relay_across, "give": do_give, "keep": do_keep,
        "finish": do_finish, "last": do_last,
    }
    for name, *which in ORDER:
        with jax.named_scope(name + "".join(str(w) for w in which)):
            run[name](*which)

    for q in range(4):
        f_pair(q).wait_send()
        for other in range(2):
            f_across(q, other).wait_send()
            for k in range(2):
                f_mate(q, other, k).wait_send()
    for j in range(chunks):
        for k in range(cols):
            d_pair(j, k).wait_send()
        for k in range(1, cols):
            d_send(j, k).wait_send()
        for g in range(2):
            y_copy(g, j).wait_send()
        m_copy(j).wait_send()
        out_copy(j).wait()


def sizes(row_count, cols, features, cotangent):
    lines = row_count // 2
    tokens = 2 * features.shape[0] * cols
    rows = features.shape[1] // lines
    width = cotangent.shape[1] // cols
    return lines, tokens, rows, width


def fused(row_count, cols, features, cotangent):
    lines, tokens, rows, width = sizes(row_count, cols, features, cotangent)
    chunks, chunk = CHUNKS, width // CHUNKS
    half = rows // 2
    dma = pltpu.SemaphoreType.DMA
    coded = pltpu.VMEM((2, chunks, half + PAD, chunk), jnp.bfloat16)
    moved = pltpu.VMEM((chunks, half + PAD, chunk), jnp.bfloat16)
    return pl.pallas_call(
        functools.partial(kernel, lines, cols),
        out_shape=jax.ShapeDtypeStruct((half, width), jnp.float32),
        in_specs=[pl.BlockSpec(memory_space=pl.ANY)] * 2,
        out_specs=pl.BlockSpec(memory_space=pl.ANY),
        scratch_shapes=[
            pltpu.VMEM((4, tokens, half), jnp.bfloat16),
            pltpu.VMEM((chunks, tokens, chunk), jnp.bfloat16),
            pltpu.VMEM((half, chunk), jnp.float32),
            coded, coded,
            pltpu.VMEM((2, chunks, half, chunk), jnp.float32),
            moved, moved,
            dma((4,)), dma((4,)), dma((4,)),
            dma((4, 2)), dma((4, 2)), dma((4, 2, 2)), dma((4, 2, 2)),
            dma((chunks,)), dma((chunks, cols)), dma((chunks, cols)),
            dma((chunks, cols)), dma((chunks, cols)),
            dma((2, chunks)), dma((2, chunks)), dma((chunks,)), dma((chunks,)),
            dma((chunks,)),
        ],
        compiler_params=pltpu.CompilerParams(
            collective_id=0, has_side_effects=True, vmem_limit_bytes=VMEM_MOST
        ),
    )(features, cotangent)


def fits(row_count, cols, features, cotangent):
    if row_count != 8 or cols != 4 or cotangent.shape[1] % (cols * CHUNKS * 128):
        return False
    if features.shape[1] % (row_count * 128) or features.shape[0] % 16:
        return False
    lines, tokens, rows, width = sizes(row_count, cols, features, cotangent)
    held = 2 * tokens * (2 * rows + width) + 11 * rows * width + 4 * rows * width // CHUNKS
    return held <= VMEM_MOST


def local(row_count, cols, features, cotangent):
    if fits(row_count, cols, features, cotangent):
        return fused(row_count, cols, features, cotangent)
    return plain(features, cotangent)


def solution(mesh):
    placed = (P(("row", "col"), None), P(("row", "col"), None))
    body = functools.partial(local, mesh.shape["row"], mesh.shape["col"])
    return jax.shard_map(
        body, mesh=mesh, in_specs=placed, out_specs=P("row", "col"), check_vma=False
    )
```

```python
import functools

import jax
import jax.numpy as jnp
from jax import lax
from jax.experimental import pallas as pl
from jax.experimental.pallas import tpu as pltpu
from jax.sharding import PartitionSpec as P

MESH = pl.DeviceIdType.MESH
CHUNKS = 8
STRIP = 32
PAD = 16
PEAK = 181.0
VMEM_MOST = 60 * 1024 * 1024


ORDER = (
    ("Z", 0), ("Z", 2), ("F", 0), ("D", 0), ("relay", 0), ("forward", "F", 0), ("P", 0),
    ("relay_across", 0), ("D", 1), ("relay", 1), ("forward", "P", 0), ("D", 2), ("relay", 2),
    ("give", 0, 0), ("relay_across", 1), ("F", 2), ("relay_across", 2), ("D", 3), ("relay", 3),
    ("forward", "F", 2), ("F", 3), ("give", 0, 1), ("relay_across", 3), ("P", 2), ("give", 0, 2),
    ("forward", "F", 3), ("D", 4), ("relay", 4), ("forward", "P", 2), ("D", 5), ("keep", 0, 0),
    ("finish", 0, 0), ("relay", 5), ("keep", 0, 2), ("keep", 0, 3), ("give", 0, 3),
    ("finish", 0, 2), ("relay_across", 4), ("D", 6), ("keep", 0, 1), ("finish", 0, 1),
    ("relay_across", 5), ("relay", 6), ("F", 1), ("relay_across", 6), ("Z", 1), ("D", 7),
    ("finish", 0, 3), ("relay", 7), ("give", 0, 4), ("forward", "F", 1), ("keep", 0, 4),
    ("relay_across", 7), ("Z", 3), ("far", 0), ("far", 1), ("far", 2), ("far", 3),
    ("give", 0, 5), ("keep", 0, 5), ("finish", 0, 4), ("far", 4), ("give", 0, 6), ("keep", 0, 6),
    ("finish", 0, 5), ("far", 5), ("P", 1), ("finish", 0, 6), ("far", 6), ("forward", "P", 1),
    ("give", 1, 0), ("give", 1, 1), ("give", 0, 7), ("keep", 0, 7), ("P", 3),
    ("forward", "P", 3), ("give", 1, 7), ("keep", 1, 7), ("keep", 1, 5), ("keep", 1, 4),
    ("keep", 1, 6), ("keep", 1, 1), ("give", 1, 2), ("finish", 0, 7), ("far", 7),
    ("finish", 1, 1), ("last", 1), ("keep", 1, 0), ("finish", 1, 0), ("give", 1, 6), ("last", 0),
    ("finish", 1, 7), ("keep", 1, 2), ("keep", 1, 3), ("give", 1, 4), ("finish", 1, 2),
    ("last", 2), ("give", 1, 3), ("finish", 1, 6), ("give", 1, 5), ("finish", 1, 4), ("last", 4),
    ("finish", 1, 3), ("last", 3), ("last", 6), ("finish", 1, 5), ("last", 5), ("last", 7),
)


def tokens_product(left, right):
    return lax.dot_general(
        left, right, (((0,), (0,)), ((), ())), preferred_element_type=jnp.float32
    )


def plain(features, cotangent):
    row_count = lax.axis_size("row")
    width_in = features.shape[1]
    local_rows = width_in // row_count
    columns = lax.all_to_all(cotangent, "col", split_axis=1, concat_axis=0, tiled=True)
    tok_local = features.shape[0]
    exchanged = lax.all_to_all(features, "row", split_axis=1, concat_axis=0, tiled=True)
    stacked = exchanged.reshape(row_count, tok_local, local_rows)
    gathered = lax.all_gather(stacked, "col", axis=1, tiled=True)
    all_tokens = gathered.reshape(-1, local_rows)
    return tokens_product(all_tokens, lax.all_gather(columns, "row", axis=0, tiled=True))


def encode(src, dst):
    rows, width = src.shape

    def strip(s):
        return pl.ds(pl.multiple_of(s * STRIP, STRIP), STRIP)

    top = lax.fori_loop(
        0, rows // STRIP, lambda s, m: jnp.maximum(m, jnp.abs(src[strip(s), :])),
        jnp.zeros((STRIP, width), jnp.float32),
    )
    top = jnp.max(top, axis=0, keepdims=True)
    undo = (jnp.maximum(top, 1e-30) * (1.0 / PEAK)).astype(jnp.bfloat16)
    dst[pl.ds(rows, PAD), :] = jnp.broadcast_to(undo, (PAD, width))
    scale = 1.0 / undo.astype(jnp.float32)

    @pl.loop(0, rows // STRIP)
    def _(s):
        t = src[strip(s), :] * scale
        u = t * t
        u = u * u
        u = u * u
        u = u * u
        dst[strip(s), :] = jnp.where(t < 0, -u, u).astype(jnp.bfloat16)


def decode_add(src, into):
    rows = into.shape[0]
    undo = src[pl.ds(rows, PAD), :].astype(jnp.float32)[:1]

    @pl.loop(0, rows // STRIP)
    def _(s):
        span = pl.ds(pl.multiple_of(s * STRIP, STRIP), STRIP)
        b = src[span, :].astype(jnp.float32)
        root = lax.rsqrt(jnp.maximum(jnp.abs(b), 1e-37))
        most = lax.rsqrt(lax.rsqrt(lax.rsqrt(root)))
        into[span, :] += (b * root) * root * most * undo


def kernel(
    lines, cols, feat, cot, out,
    fall, dall, tmp, ysend, yrecv, acc, msend, mrecv,
    fl, fz_s, fz_r, fx_s, fx_r, fm_s, fm_r,
    dl, dx_s, dx_r, dz_s, dz_r, y_s, y_r, m_s, m_r, o_s,
):
    row = lax.axis_index("row")
    col = lax.axis_index("col")
    z, y = row // 2, row % 2
    here = z % 2
    near = z + 1 - 2 * here
    far = lines - 1 - z
    inner = (z > 0) & (z < lines - 1)
    tok = feat.shape[0]
    half = fall.shape[2]
    chunks, _, chunk = dall.shape
    width = chunks * chunk

    def at_row(zz, yy):
        return {"row": zz * 2 + yy, "col": col}

    pair, mirror, partner = at_row(near, y), at_row(far, y), at_row(z, 1 - y)
    mate_col = col + 1 - 2 * (col % 2)
    col_of = (col, mate_col, (col + 2) % cols, (mate_col + 2) % cols)
    MATE, ACROSS = 1, 2

    def at_col(k):
        return {"row": row, "col": col_of[k]}

    def remote(src, dst, s, r, dev):
        return pltpu.make_async_remote_copy(
            src_ref=src, dst_ref=dst, send_sem=s, recv_sem=r,
            device_id=dev, device_id_type=MESH,
        )

    barrier = pltpu.get_barrier_semaphore()
    others = [pair, mirror, partner] + [at_col(k) for k in range(1, cols)]
    for dev in others:
        pl.semaphore_signal(barrier, inc=1, device_id=dev, device_id_type=MESH)
    pl.semaphore_wait(barrier, len(others))

    def slot(plane, c):
        return pl.ds(pl.multiple_of((plane * cols + c) * tok, tok), tok)

    def f_cols(zz, q):
        wanted = lines - 1 - zz if q % 2 == 0 else zz
        yy = 1 - y if q < 2 else y
        return feat.at[:, pl.ds(pl.multiple_of((wanted * 2 + yy) * half, half), half)]

    def f_own(q):
        return pltpu.make_async_copy(f_cols(z, q), fall.at[q, slot(here, col)], fl.at[q])

    def f_pair(q):
        return remote(f_cols(near, q), fall.at[q, slot(here, col)], fz_s.at[q], fz_r.at[q], pair)

    def f_block(q, other, k):
        return fall.at[q, slot(1 - here if other else here, col_of[k])]

    def f_across(q, other):
        block = f_block(q, other, 0)
        src = block if other else f_cols(z, q)
        return remote(src, block, fx_s.at[q, other], fx_r.at[q, other], at_col(ACROSS))

    def f_mate(q, other, k):
        block = f_block(q, other, ACROSS * k)
        src = f_cols(z, q) if not other and not k else block
        return remote(src, block, fm_s.at[q, other, k], fm_r.at[q, other, k], at_col(MATE))

    def d_cols(cc, j):
        return cot.at[:, pl.ds(pl.multiple_of(cc * width + j * chunk, chunk), chunk)]

    def d_own(j):
        return pltpu.make_async_copy(d_cols(col, j), dall.at[j, slot(here, col)], dl.at[j])

    def d_send(j, k):
        return remote(
            d_cols(col_of[k], j), dall.at[j, slot(here, col)],
            dx_s.at[j, k], dx_r.at[j, k], at_col(k),
        )

    def d_pair(j, k):
        block = dall.at[j, slot(here, col_of[k])]
        return remote(
            block if k else d_cols(col, j), block, dz_s.at[j, k], dz_r.at[j, k], pair
        )

    def y_copy(g, j):
        return remote(ysend.at[g, j], yrecv.at[g, j], y_s.at[g, j], y_r.at[g, j], partner)

    def m_copy(j):
        return remote(msend.at[j], mrecv.at[j], m_s.at[j], m_r.at[j], mirror)

    def out_copy(j):
        return pltpu.make_async_copy(acc.at[1, j], out.at[:, pl.ds(j * chunk, chunk)], o_s.at[j])

    ready = set()

    def once(key):
        new = key not in ready
        ready.add(key)
        return new

    def arrive(q, j):
        if once(("F", q)):
            f_own(q).wait()
            for other in range(2):
                for k in range(2):
                    f_mate(q, other, k).wait_recv()
        if once(("D", j)):
            d_own(j).wait()
            for k in range(cols):
                d_pair(j, k).wait_recv()

    def do_Z(q):
        f_pair(q).start()

    def do_F(q):
        f_across(q, 0).start()
        f_mate(q, 0, 0).start()
        f_own(q).start()

    def do_P(q):
        f_pair(q).wait_recv()
        f_across(q, 1).start()
        f_mate(q, 1, 0).start()

    def do_D(j):
        d_pair(j, 0).start()
        for k in (2, 3, 1):
            d_send(j, k).start()
        d_own(j).start()

    def do_forward(kind, q):
        other = 1 if kind == "P" else 0
        f_across(q, other).wait_recv()
        f_mate(q, other, 1).start()

    def do_relay(j):
        d_send(j, MATE).wait_recv()
        d_pair(j, MATE).start()

    def do_relay_across(j):
        for k in (2, 3):
            d_send(j, k).wait_recv()
            d_pair(j, k).start()

    def do_give(g, j):
        arrive(g, j)
        tmp[...] = tokens_product(fall[g], dall[j])
        encode(tmp, ysend.at[g, j])
        y_copy(g, j).start()

    def do_keep(g, j):
        arrive(2 + g, j)
        acc[g, j] = tokens_product(fall[2 + g], dall[j])

    def do_finish(g, j):
        y_copy(g, j).wait_recv()
        decode_add(yrecv.at[g, j], acc.at[g, j])
        if g == 0:
            encode(acc.at[0, j], msend.at[j])

            @pl.when(inner)
            def _():
                m_copy(j).start()

    def do_far(j):
        @pl.when(~inner)
        def _():
            m_copy(j).start()

    def do_last(j):
        m_copy(j).wait_recv()
        decode_add(mrecv.at[j], acc.at[1, j])
        out_copy(j).start()

    run = {
        "Z": do_Z, "F": do_F, "P": do_P, "far": do_far, "D": do_D, "forward": do_forward, "relay": do_relay,
        "relay_across": do_relay_across, "give": do_give, "keep": do_keep,
        "finish": do_finish, "last": do_last,
    }
    for name, *which in ORDER:
        with jax.named_scope(name + "".join(str(w) for w in which)):
            run[name](*which)

    for q in range(4):
        f_pair(q).wait_send()
        for other in range(2):
            f_across(q, other).wait_send()
            for k in range(2):
                f_mate(q, other, k).wait_send()
    for j in range(chunks):
        for k in range(cols):
            d_pair(j, k).wait_send()
        for k in range(1, cols):
            d_send(j, k).wait_send()
        for g in range(2):
            y_copy(g, j).wait_send()
        m_copy(j).wait_send()
        out_copy(j).wait()


def sizes(row_count, cols, features, cotangent):
    lines = row_count // 2
    tokens = 2 * features.shape[0] * cols
    rows = features.shape[1] // lines
    width = cotangent.shape[1] // cols
    return lines, tokens, rows, width


def fused(row_count, cols, features, cotangent):
    lines, tokens, rows, width = sizes(row_count, cols, features, cotangent)
    chunks, chunk = CHUNKS, width // CHUNKS
    half = rows // 2
    dma = pltpu.SemaphoreType.DMA
    coded = pltpu.VMEM((2, chunks, half + PAD, chunk), jnp.bfloat16)
    moved = pltpu.VMEM((chunks, half + PAD, chunk), jnp.bfloat16)
    return pl.pallas_call(
        functools.partial(kernel, lines, cols),
        out_shape=jax.ShapeDtypeStruct((half, width), jnp.float32),
        in_specs=[pl.BlockSpec(memory_space=pl.ANY)] * 2,
        out_specs=pl.BlockSpec(memory_space=pl.ANY),
        scratch_shapes=[
            pltpu.VMEM((4, tokens, half), jnp.bfloat16),
            pltpu.VMEM((chunks, tokens, chunk), jnp.bfloat16),
            pltpu.VMEM((half, chunk), jnp.float32),
            coded, coded,
            pltpu.VMEM((2, chunks, half, chunk), jnp.float32),
            moved, moved,
            dma((4,)), dma((4,)), dma((4,)),
            dma((4, 2)), dma((4, 2)), dma((4, 2, 2)), dma((4, 2, 2)),
            dma((chunks,)), dma((chunks, cols)), dma((chunks, cols)),
            dma((chunks, cols)), dma((chunks, cols)),
            dma((2, chunks)), dma((2, chunks)), dma((chunks,)), dma((chunks,)),
            dma((chunks,)),
        ],
        compiler_params=pltpu.CompilerParams(
            collective_id=0, has_side_effects=True, vmem_limit_bytes=VMEM_MOST
        ),
    )(features, cotangent)


def fits(row_count, cols, features, cotangent):
    if row_count != 8 or cols != 4 or cotangent.shape[1] % (cols * CHUNKS * 128):
        return False
    if features.shape[1] % (row_count * 128) or features.shape[0] % 16:
        return False
    lines, tokens, rows, width = sizes(row_count, cols, features, cotangent)
    held = 2 * tokens * (2 * rows + width) + 11 * rows * width + 4 * rows * width // CHUNKS
    return held <= VMEM_MOST


def local(row_count, cols, features, cotangent):
    if fits(row_count, cols, features, cotangent):
        return fused(row_count, cols, features, cotangent)
    return plain(features, cotangent)


def solution(mesh):
    placed = (P(("row", "col"), None), P(("row", "col"), None))
    body = functools.partial(local, mesh.shape["row"], mesh.shape["col"])
    return jax.shard_map(
        body, mesh=mesh, in_specs=placed, out_specs=P("row", "col"), check_vma=False
    )
```

```python
import functools

import jax
import jax.numpy as jnp
from jax import lax
from jax.experimental import pallas as pl
from jax.experimental.pallas import tpu as pltpu
from jax.sharding import PartitionSpec as P

MESH = pl.DeviceIdType.MESH
WIDTHS = (1, 1, 1, 1, 1, 1, 1, 1)
PARTS = sum(WIDTHS)
STRIP = 32
PEAK = 181.0
VMEM_MOST = 58 * 1024 * 1024


ORDER = (
    ("Z", 0), ("Z", 2), ("F", 0), ("D", 0), ("relay", 0), ("forward", "F", 0), ("P", 0),
    ("relay_across", 0), ("D", 1), ("relay", 1), ("forward", "P", 0), ("D", 2), ("relay", 2),
    ("give", 0, 0), ("relay_across", 1), ("D", 3), ("relay", 3), ("relay_across", 2), ("D", 4),
    ("relay", 4), ("relay_across", 3), ("F", 2), ("give", 0, 1), ("relay_across", 4), ("P", 2),
    ("forward", "F", 2), ("D", 5), ("relay", 5), ("give", 0, 2), ("forward", "P", 2), ("F", 3),
    ("keep", 0, 2), ("keep", 0, 1), ("relay_across", 5), ("D", 6), ("finish", 0, 1),
    ("keep", 0, 0), ("finish", 0, 0), ("relay", 6), ("forward", "F", 3), ("F", 1),
    ("give", 0, 3), ("finish", 0, 2), ("keep", 0, 3), ("relay_across", 6), ("give", 0, 4),
    ("Z", 1), ("Z", 3), ("D", 7), ("keep", 0, 4), ("relay", 7), ("forward", "F", 1),
    ("finish", 0, 3), ("relay_across", 7), ("give", 0, 5), ("far", 0), ("far", 1), ("far", 2),
    ("far", 3), ("keep", 0, 5), ("finish", 0, 4), ("far", 4), ("give", 0, 6), ("finish", 0, 5),
    ("far", 5), ("keep", 0, 6), ("P", 1), ("P", 3), ("finish", 0, 6), ("far", 6),
    ("forward", "P", 1), ("give", 1, 6), ("forward", "P", 3), ("keep", 1, 0), ("give", 0, 7),
    ("keep", 0, 7), ("keep", 1, 5), ("keep", 1, 7), ("keep", 1, 3), ("keep", 1, 4),
    ("give", 1, 1), ("keep", 1, 2), ("keep", 1, 6), ("finish", 0, 7), ("far", 7),
    ("finish", 1, 6), ("keep", 1, 1), ("give", 1, 3), ("finish", 1, 1), ("last", 1),
    ("give", 1, 7), ("finish", 1, 3), ("give", 1, 4), ("finish", 1, 7), ("give", 1, 0),
    ("last", 3), ("finish", 1, 4), ("give", 1, 5), ("last", 4), ("finish", 1, 0), ("last", 0),
    ("give", 1, 2), ("finish", 1, 5), ("last", 5), ("last", 6), ("finish", 1, 2), ("last", 2),
    ("last", 7),
)


def tokens_product(left, right):
    return lax.dot_general(
        left, right, (((0,), (0,)), ((), ())), preferred_element_type=jnp.float32
    )


def plain(features, cotangent):
    row_count = lax.axis_size("row")
    width_in = features.shape[1]
    local_rows = width_in // row_count
    columns = lax.all_to_all(cotangent, "col", split_axis=1, concat_axis=0, tiled=True)
    tok_local = features.shape[0]
    exchanged = lax.all_to_all(features, "row", split_axis=1, concat_axis=0, tiled=True)
    stacked = exchanged.reshape(row_count, tok_local, local_rows)
    gathered = lax.all_gather(stacked, "col", axis=1, tiled=True)
    all_tokens = gathered.reshape(-1, local_rows)
    return tokens_product(all_tokens, lax.all_gather(columns, "row", axis=0, tiled=True))


def encode(src, dst, undo_row):
    rows, width = src.shape

    def strip(s):
        return pl.ds(pl.multiple_of(s * STRIP, STRIP), STRIP)

    top = lax.fori_loop(
        0, rows // STRIP, lambda s, m: jnp.maximum(m, jnp.abs(src[strip(s), :])),
        jnp.zeros((STRIP, width), jnp.float32),
    )
    undo = jnp.maximum(jnp.max(top, axis=0, keepdims=True), 1e-30) * (1.0 / PEAK)
    undo_row[...] = undo
    scale = 1.0 / undo

    @pl.loop(0, rows // STRIP)
    def _(s):
        t = src[strip(s), :] * scale
        u = t * t
        u = u * u
        u = u * u
        u = u * u
        dst[strip(s), :] = jnp.where(t < 0, -u, u).astype(jnp.bfloat16)


def decode_add(src, undo_row, into):
    undo = undo_row[...]

    @pl.loop(0, into.shape[0] // STRIP)
    def _(s):
        span = pl.ds(pl.multiple_of(s * STRIP, STRIP), STRIP)
        b = src[span, :].astype(jnp.float32)
        root = lax.rsqrt(jnp.maximum(jnp.abs(b), 1e-37))
        most = lax.rsqrt(lax.rsqrt(lax.rsqrt(root)))
        into[span, :] += (b * root) * root * most * undo


def kernel(
    lines, cols, feat, cot, out,
    fall, dall, tmp, ysend, yrecv, yu_out, yu_in, acc, msend, mrecv, mu_out, mu_in,
    fl, fz_s, fz_r, fx_s, fx_r, fm_s, fm_r,
    dl, dx_s, dx_r, dz_s, dz_r, y_s, y_r, yu_s, yu_r, m_s, m_r, mu_s, mu_r,
):
    row = lax.axis_index("row")
    col = lax.axis_index("col")
    z, y = row // 2, row % 2
    here = z % 2
    near = z + 1 - 2 * here
    far = lines - 1 - z
    inner = (z > 0) & (z < lines - 1)
    tok = feat.shape[0]
    half = fall.shape[2]
    chunks = len(WIDTHS)
    width = dall.shape[1]
    part = width // PARTS

    def cols_of(j):
        return pl.ds(sum(WIDTHS[:j]) * part, WIDTHS[j] * part)


    def at_row(zz, yy):
        return {"row": zz * 2 + yy, "col": col}

    pair, mirror, partner = at_row(near, y), at_row(far, y), at_row(z, 1 - y)
    mate_col = col + 1 - 2 * (col % 2)
    col_of = (col, mate_col, (col + 2) % cols, (mate_col + 2) % cols)
    MATE, ACROSS = 1, 2

    def at_col(k):
        return {"row": row, "col": col_of[k]}

    def remote(src, dst, s, r, dev):
        return pltpu.make_async_remote_copy(
            src_ref=src, dst_ref=dst, send_sem=s, recv_sem=r,
            device_id=dev, device_id_type=MESH,
        )

    barrier = pltpu.get_barrier_semaphore()
    others = [pair, mirror, partner] + [at_col(k) for k in range(1, cols)]
    for dev in others:
        pl.semaphore_signal(barrier, inc=1, device_id=dev, device_id_type=MESH)
    pl.semaphore_wait(barrier, len(others))

    def slot(plane, c):
        return pl.ds(pl.multiple_of((plane * cols + c) * tok, tok), tok)

    def f_cols(zz, q):
        wanted = lines - 1 - zz if q % 2 == 0 else zz
        yy = 1 - y if q < 2 else y
        return feat.at[:, pl.ds(pl.multiple_of((wanted * 2 + yy) * half, half), half)]

    def f_own(q):
        return pltpu.make_async_copy(f_cols(z, q), fall.at[q, slot(here, col)], fl.at[q])

    def f_pair(q):
        return remote(f_cols(near, q), fall.at[q, slot(here, col)], fz_s.at[q], fz_r.at[q], pair)

    def f_block(q, other, k):
        return fall.at[q, slot(1 - here if other else here, col_of[k])]

    def f_across(q, other):
        block = f_block(q, other, 0)
        src = block if other else f_cols(z, q)
        return remote(src, block, fx_s.at[q, other], fx_r.at[q, other], at_col(ACROSS))

    def f_mate(q, other, k):
        block = f_block(q, other, ACROSS * k)
        src = f_cols(z, q) if not other and not k else block
        return remote(src, block, fm_s.at[q, other, k], fm_r.at[q, other, k], at_col(MATE))

    def d_cols(cc, j):
        first = pl.multiple_of(cc * width + sum(WIDTHS[:j]) * part, part)
        return cot.at[:, pl.ds(first, WIDTHS[j] * part)]

    def d_own(j):
        return pltpu.make_async_copy(d_cols(col, j), dall.at[slot(here, col), cols_of(j)], dl.at[j])

    def d_send(j, k):
        return remote(
            d_cols(col_of[k], j), dall.at[slot(here, col), cols_of(j)],
            dx_s.at[j, k], dx_r.at[j, k], at_col(k),
        )

    def d_pair(j, k):
        block = dall.at[slot(here, col_of[k]), cols_of(j)]
        return remote(
            block if k else d_cols(col, j), block, dz_s.at[j, k], dz_r.at[j, k], pair
        )

    def y_copies(g, j):
        c = cols_of(j)
        return (
            remote(yu_out.at[g, :, c], yu_in.at[g, :, c], yu_s.at[g, j], yu_r.at[g, j], partner),
            remote(ysend.at[g, :, c], yrecv.at[g, :, c], y_s.at[g, j], y_r.at[g, j], partner),
        )

    def m_copies(j):
        c = cols_of(j)
        return (
            remote(mu_out.at[:, c], mu_in.at[:, c], mu_s.at[j], mu_r.at[j], mirror),
            remote(msend.at[:, c], mrecv.at[:, c], m_s.at[j], m_r.at[j], mirror),
        )

    def start(copies):
        for copy in copies:
            copy.start()

    def receive(copies):
        for copy in copies:
            copy.wait_recv()

    def total(g, j):
        return (out if g else acc).at[:, cols_of(j)]

    ready = set()

    def once(key):
        new = key not in ready
        ready.add(key)
        return new

    def arrive(q, j):
        if once(("F", q)):
            f_own(q).wait()
            for other in range(2):
                for k in range(2):
                    f_mate(q, other, k).wait_recv()
        if once(("D", j)):
            d_own(j).wait()
            for k in range(cols):
                d_pair(j, k).wait_recv()

    def do_Z(q):
        f_pair(q).start()

    def do_F(q):
        f_across(q, 0).start()
        f_mate(q, 0, 0).start()
        f_own(q).start()

    def do_P(q):
        f_pair(q).wait_recv()
        f_across(q, 1).start()
        f_mate(q, 1, 0).start()

    def do_D(j):
        d_pair(j, 0).start()
        for k in (2, 3, 1):
            d_send(j, k).start()
        d_own(j).start()

    def do_forward(kind, q):
        other = 1 if kind == "P" else 0
        f_across(q, other).wait_recv()
        f_mate(q, other, 1).start()

    def do_relay(j):
        d_send(j, MATE).wait_recv()
        d_pair(j, MATE).start()

    def do_relay_across(j):
        for k in (2, 3):
            d_send(j, k).wait_recv()
            d_pair(j, k).start()

    def do_give(g, j):
        arrive(g, j)
        c = cols_of(j)
        made = tmp.at[:, pl.ds(0, c.size)]
        made[...] = tokens_product(fall[g], dall[:, c])
        encode(made, ysend.at[g, :, c], yu_out.at[g, :, c])
        start(y_copies(g, j))

    def do_keep(g, j):
        arrive(2 + g, j)
        total(g, j)[...] = tokens_product(fall[2 + g], dall[:, cols_of(j)])

    def do_finish(g, j):
        receive(y_copies(g, j))
        c = cols_of(j)
        decode_add(yrecv.at[g, :, c], yu_in.at[g, :, c], total(g, j))
        if g == 0:
            encode(total(0, j), msend.at[:, c], mu_out.at[:, c])

            @pl.when(inner)
            def _():
                start(m_copies(j))

    def do_far(j):
        @pl.when(~inner)
        def _():
            start(m_copies(j))

    def do_last(j):
        receive(m_copies(j))
        c = cols_of(j)
        decode_add(mrecv.at[:, c], mu_in.at[:, c], total(1, j))

    run = {
        "Z": do_Z, "F": do_F, "P": do_P, "far": do_far, "D": do_D, "forward": do_forward, "relay": do_relay,
        "relay_across": do_relay_across, "give": do_give, "keep": do_keep,
        "finish": do_finish, "last": do_last,
    }
    for name, *which in ORDER:
        with jax.named_scope(name + "".join(str(w) for w in which)):
            run[name](*which)

    for q in range(4):
        f_pair(q).wait_send()
        for other in range(2):
            f_across(q, other).wait_send()
            for k in range(2):
                f_mate(q, other, k).wait_send()
    for j in range(chunks):
        for k in range(cols):
            d_pair(j, k).wait_send()
        for k in range(1, cols):
            d_send(j, k).wait_send()
        for copy in y_copies(0, j) + y_copies(1, j) + m_copies(j):
            copy.wait_send()


def sizes(row_count, cols, features, cotangent):
    lines = row_count // 2
    tokens = 2 * features.shape[0] * cols
    rows = features.shape[1] // lines
    width = cotangent.shape[1] // cols
    return lines, tokens, rows, width


def fused(row_count, cols, features, cotangent):
    lines, tokens, rows, width = sizes(row_count, cols, features, cotangent)
    chunks, half = len(WIDTHS), rows // 2
    dma = pltpu.SemaphoreType.DMA
    coded = pltpu.VMEM((2, half, width), jnp.bfloat16)
    moved = pltpu.VMEM((half, width), jnp.bfloat16)
    coded_undo = pltpu.VMEM((2, 1, width), jnp.float32)
    moved_undo = pltpu.VMEM((1, width), jnp.float32)
    return pl.pallas_call(
        functools.partial(kernel, lines, cols),
        out_shape=pltpu.VMEM((half, width), jnp.float32),
        in_specs=[pl.BlockSpec(memory_space=pl.ANY)] * 2,
        out_specs=pl.BlockSpec(memory_space=pltpu.VMEM),
        scratch_shapes=[
            pltpu.VMEM((4, tokens, half), jnp.bfloat16),
            pltpu.VMEM((tokens, width), jnp.bfloat16),
            pltpu.VMEM((half, max(WIDTHS) * width // PARTS), jnp.float32),
            coded, coded, coded_undo, coded_undo,
            pltpu.VMEM((half, width), jnp.float32),
            moved, moved, moved_undo, moved_undo,
            dma((4,)), dma((4,)), dma((4,)),
            dma((4, 2)), dma((4, 2)), dma((4, 2, 2)), dma((4, 2, 2)),
            dma((chunks,)), dma((chunks, cols)), dma((chunks, cols)),
            dma((chunks, cols)), dma((chunks, cols)),
            dma((2, chunks)), dma((2, chunks)), dma((2, chunks)), dma((2, chunks)),
            dma((chunks,)), dma((chunks,)), dma((chunks,)), dma((chunks,)),
        ],
        compiler_params=pltpu.CompilerParams(
            collective_id=0, has_side_effects=True, vmem_limit_bytes=VMEM_MOST
        ),
    )(features, cotangent)


def fits(row_count, cols, features, cotangent):
    if row_count != 8 or cols != 4 or cotangent.shape[1] % (cols * PARTS * 128):
        return False
    if features.shape[1] % (row_count * 128) or features.shape[0] % 16:
        return False
    lines, tokens, rows, width = sizes(row_count, cols, features, cotangent)
    held = 2 * tokens * (2 * rows + width) + 11 * rows * width + 4 * rows * width // 8
    return held <= VMEM_MOST


def local(row_count, cols, features, cotangent):
    if fits(row_count, cols, features, cotangent):
        return fused(row_count, cols, features, cotangent)
    return plain(features, cotangent)


def solution(mesh):
    placed = (P(("row", "col"), None), P(("row", "col"), None))
    body = functools.partial(local, mesh.shape["row"], mesh.shape["col"])
    return jax.shard_map(
        body, mesh=mesh, in_specs=placed, out_specs=P("row", "col"), check_vma=False
    )
```

```python
import functools

import jax
import jax.numpy as jnp
from jax import lax
from jax.experimental import pallas as pl
from jax.experimental.pallas import tpu as pltpu
from jax.sharding import PartitionSpec as P

MESH = pl.DeviceIdType.MESH
WIDTHS = (1, 1, 1, 1, 1, 1, 1, 1)
PARTS = sum(WIDTHS)
STRIP = 32
PEAK = 181.0
VMEM_MOST = 58 * 1024 * 1024


ORDER = (
    ("Z", 0), ("Z", 2), ("F", 0), ("D", 0), ("relay", 0), ("forward", "F", 0), ("P", 0),
    ("relay_across", 0), ("D", 1), ("relay", 1), ("forward", "P", 0), ("D", 2), ("relay", 2),
    ("give", 0, 0), ("relay_across", 1), ("D", 3), ("relay", 3), ("relay_across", 2), ("D", 4),
    ("relay", 4), ("relay_across", 3), ("F", 2), ("give", 0, 1), ("relay_across", 4), ("P", 2),
    ("forward", "F", 2), ("D", 5), ("relay", 5), ("give", 0, 2), ("forward", "P", 2), ("F", 3),
    ("keep", 0, 2), ("keep", 0, 1), ("relay_across", 5), ("D", 6), ("finish", 0, 1),
    ("keep", 0, 0), ("finish", 0, 0), ("relay", 6), ("forward", "F", 3), ("F", 1),
    ("give", 0, 3), ("finish", 0, 2), ("keep", 0, 3), ("relay_across", 6), ("give", 0, 4),
    ("Z", 1), ("Z", 3), ("D", 7), ("keep", 0, 4), ("relay", 7), ("forward", "F", 1),
    ("finish", 0, 3), ("relay_across", 7), ("give", 0, 5), ("far", 0), ("far", 1), ("far", 2),
    ("far", 3), ("keep", 0, 5), ("finish", 0, 4), ("far", 4), ("give", 0, 6), ("finish", 0, 5),
    ("far", 5), ("keep", 0, 6), ("P", 1), ("P", 3), ("finish", 0, 6), ("far", 6),
    ("forward", "P", 1), ("give", 1, 6), ("forward", "P", 3), ("keep", 1, 0), ("give", 0, 7),
    ("keep", 0, 7), ("keep", 1, 5), ("keep", 1, 7), ("keep", 1, 3), ("keep", 1, 4),
    ("give", 1, 1), ("keep", 1, 2), ("keep", 1, 6), ("finish", 0, 7), ("far", 7),
    ("finish", 1, 6), ("keep", 1, 1), ("give", 1, 3), ("finish", 1, 1), ("last", 1),
    ("give", 1, 7), ("finish", 1, 3), ("give", 1, 4), ("finish", 1, 7), ("give", 1, 0),
    ("last", 3), ("finish", 1, 4), ("give", 1, 5), ("last", 4), ("finish", 1, 0), ("last", 0),
    ("give", 1, 2), ("finish", 1, 5), ("last", 5), ("last", 6), ("finish", 1, 2), ("last", 2),
    ("last", 7),
)


def tokens_product(left, right):
    return lax.dot_general(
        left, right, (((0,), (0,)), ((), ())), preferred_element_type=jnp.float32
    )


def plain(features, cotangent):
    row_count = lax.axis_size("row")
    width_in = features.shape[1]
    local_rows = width_in // row_count
    columns = lax.all_to_all(cotangent, "col", split_axis=1, concat_axis=0, tiled=True)
    tok_local = features.shape[0]
    exchanged = lax.all_to_all(features, "row", split_axis=1, concat_axis=0, tiled=True)
    stacked = exchanged.reshape(row_count, tok_local, local_rows)
    gathered = lax.all_gather(stacked, "col", axis=1, tiled=True)
    all_tokens = gathered.reshape(-1, local_rows)
    return tokens_product(all_tokens, lax.all_gather(columns, "row", axis=0, tiled=True))


def encode(src, dst, undo_row):
    rows, width = src.shape

    def strip(s):
        return pl.ds(pl.multiple_of(s * STRIP, STRIP), STRIP)

    top = lax.fori_loop(
        0, rows // STRIP, lambda s, m: jnp.maximum(m, jnp.abs(src[strip(s), :])),
        jnp.zeros((STRIP, width), jnp.float32),
    )
    undo = jnp.maximum(jnp.max(top, axis=0, keepdims=True), 1e-30) * (1.0 / PEAK)
    undo_row[...] = undo
    scale = 1.0 / undo

    @pl.loop(0, rows // STRIP)
    def _(s):
        t = src[strip(s), :] * scale
        u = t * t
        u = u * u
        u = u * u
        u = u * u
        dst[strip(s), :] = jnp.where(t < 0, -u, u).astype(jnp.bfloat16)


def decode_add(src, undo_row, into):
    undo = undo_row[...]

    @pl.loop(0, into.shape[0] // STRIP)
    def _(s):
        span = pl.ds(pl.multiple_of(s * STRIP, STRIP), STRIP)
        b = src[span, :].astype(jnp.float32)
        root = lax.rsqrt(jnp.maximum(jnp.abs(b), 1e-37))
        most = lax.rsqrt(lax.rsqrt(lax.rsqrt(root)))
        into[span, :] += (b * root) * root * most * undo


def kernel(
    lines, cols, feat, cot, out,
    fall, dall, tmp, ysend, yrecv, yu_out, yu_in, acc, msend, mrecv, mu_out, mu_in,
    f_s, fz_r, fx_r, fm_r, d_s, dx_r, dz_r, y_s, y_r, yu_s, yu_r, m_s, m_r, mu_s, mu_r,
):
    row = lax.axis_index("row")
    col = lax.axis_index("col")
    z, y = row // 2, row % 2
    here = z % 2
    near = z + 1 - 2 * here
    far = lines - 1 - z
    inner = (z > 0) & (z < lines - 1)
    tok = feat.shape[0]
    half = fall.shape[2]
    chunks = len(WIDTHS)
    width = dall.shape[1]
    part = width // PARTS

    def cols_of(j):
        return pl.ds(sum(WIDTHS[:j]) * part, WIDTHS[j] * part)


    def at_row(zz, yy):
        return {"row": zz * 2 + yy, "col": col}

    pair, mirror, partner = at_row(near, y), at_row(far, y), at_row(z, 1 - y)
    mate_col = col + 1 - 2 * (col % 2)
    col_of = (col, mate_col, (col + 2) % cols, (mate_col + 2) % cols)
    MATE, ACROSS = 1, 2

    def at_col(k):
        return {"row": row, "col": col_of[k]}

    def remote(src, dst, s, r, dev):
        return pltpu.make_async_remote_copy(
            src_ref=src, dst_ref=dst, send_sem=s, recv_sem=r,
            device_id=dev, device_id_type=MESH,
        )

    barrier = pltpu.get_barrier_semaphore()
    others = [pair, mirror, partner] + [at_col(k) for k in range(1, cols)]
    for dev in others:
        pl.semaphore_signal(barrier, inc=1, device_id=dev, device_id_type=MESH)
    pl.semaphore_wait(barrier, len(others))

    def slot(plane, c):
        return pl.ds(pl.multiple_of((plane * cols + c) * tok, tok), tok)

    def f_cols(zz, q):
        wanted = lines - 1 - zz if q % 2 == 0 else zz
        yy = 1 - y if q < 2 else y
        return feat.at[:, pl.ds(pl.multiple_of((wanted * 2 + yy) * half, half), half)]

    def f_own(q):
        return pltpu.make_async_copy(f_cols(z, q), fall.at[q, slot(here, col)], fm_r.at[q])

    def f_pair(q):
        return remote(f_cols(near, q), fall.at[q, slot(here, col)], f_s.at[0], fz_r.at[q], pair)

    def f_block(q, other, k):
        return fall.at[q, slot(1 - here if other else here, col_of[k])]

    def f_across(q, other):
        block = f_block(q, other, 0)
        src = block if other else f_cols(z, q)
        return remote(src, block, f_s.at[0], fx_r.at[q, other], at_col(ACROSS))

    def f_mate(q, other, k):
        block = f_block(q, other, ACROSS * k)
        src = f_cols(z, q) if not other and not k else block
        return remote(src, block, f_s.at[0], fm_r.at[q], at_col(MATE))

    def d_cols(cc, j):
        first = pl.multiple_of(cc * width + sum(WIDTHS[:j]) * part, part)
        return cot.at[:, pl.ds(first, WIDTHS[j] * part)]

    def d_own(j):
        return pltpu.make_async_copy(d_cols(col, j), dall.at[slot(here, col), cols_of(j)], dz_r.at[j])

    def d_send(j, k):
        return remote(
            d_cols(col_of[k], j), dall.at[slot(here, col), cols_of(j)],
            d_s.at[0], dx_r.at[j, k // ACROSS], at_col(k),
        )

    def d_block(j, k):
        if k < ACROSS:
            return dall.at[slot(here, col_of[k]), cols_of(j)]
        first = (here * cols + (col // 2 * 2 + 2) % cols) * tok
        return dall.at[pl.ds(pl.multiple_of(first, tok), 2 * tok), cols_of(j)]

    def d_recv(j, k):
        block = d_block(j, k)
        return remote(block, block, d_s.at[0], dx_r.at[j, k // ACROSS], at_col(k))

    def d_pair(j, k):
        block = d_block(j, k)
        return remote(block if k else d_cols(col, j), block, d_s.at[0], dz_r.at[j], pair)

    def bytes_of(block, sem):
        return pltpu.make_async_copy(block, block, sem)

    def y_copies(g, j):
        c = cols_of(j)
        return (
            remote(yu_out.at[g, :, c], yu_in.at[g, :, c], yu_s.at[0], yu_r.at[g, j], partner),
            remote(ysend.at[g, :, c], yrecv.at[g, :, c], y_s.at[0], y_r.at[g, j], partner),
        )

    def m_copies(j):
        c = cols_of(j)
        return (
            remote(mu_out.at[:, c], mu_in.at[:, c], mu_s.at[0], mu_r.at[j], mirror),
            remote(msend.at[:, c], mrecv.at[:, c], m_s.at[0], m_r.at[j], mirror),
        )

    def start(copies):
        for copy in copies:
            copy.start()

    def receive(copies):
        for copy in copies:
            copy.wait_recv()

    def total(g, j):
        return (out if g else acc).at[:, cols_of(j)]

    ready = set()

    def once(key):
        new = key not in ready
        ready.add(key)
        return new

    def arrive(q, j):
        if once(("F", q)):
            bytes_of(fall.at[q, pl.ds(0, 5 * tok)], fm_r.at[q]).wait()
        if once(("D", j)):
            bytes_of(dall.at[pl.ds(0, 5 * tok), cols_of(j)], dz_r.at[j]).wait()

    def do_Z(q):
        f_pair(q).start()

    def do_F(q):
        f_across(q, 0).start()
        f_mate(q, 0, 0).start()
        f_own(q).start()

    def do_P(q):
        f_pair(q).wait_recv()
        f_across(q, 1).start()
        f_mate(q, 1, 0).start()

    def do_D(j):
        d_pair(j, 0).start()
        for k in (2, 3, 1):
            d_send(j, k).start()
        d_own(j).start()

    def do_forward(kind, q):
        other = 1 if kind == "P" else 0
        f_across(q, other).wait_recv()
        f_mate(q, other, 1).start()

    def do_relay(j):
        d_recv(j, MATE).wait_recv()
        d_pair(j, MATE).start()

    def do_relay_across(j):
        d_recv(j, ACROSS).wait_recv()
        d_pair(j, ACROSS).start()

    def do_give(g, j):
        arrive(g, j)
        c = cols_of(j)
        made = tmp.at[:, pl.ds(0, c.size)]
        made[...] = tokens_product(fall[g], dall[:, c])
        encode(made, ysend.at[g, :, c], yu_out.at[g, :, c])
        start(y_copies(g, j))

    def do_keep(g, j):
        arrive(2 + g, j)
        total(g, j)[...] = tokens_product(fall[2 + g], dall[:, cols_of(j)])

    def do_finish(g, j):
        receive(y_copies(g, j))
        c = cols_of(j)
        decode_add(yrecv.at[g, :, c], yu_in.at[g, :, c], total(g, j))
        if g == 0:
            encode(total(0, j), msend.at[:, c], mu_out.at[:, c])

            @pl.when(inner)
            def _():
                start(m_copies(j))

    def do_far(j):
        @pl.when(~inner)
        def _():
            start(m_copies(j))

    def do_last(j):
        receive(m_copies(j))
        c = cols_of(j)
        decode_add(mrecv.at[:, c], mu_in.at[:, c], total(1, j))

    run = {
        "Z": do_Z, "F": do_F, "P": do_P, "far": do_far, "D": do_D, "forward": do_forward, "relay": do_relay,
        "relay_across": do_relay_across, "give": do_give, "keep": do_keep,
        "finish": do_finish, "last": do_last,
    }
    for name, *which in ORDER:
        with jax.named_scope(name + "".join(str(w) for w in which)):
            run[name](*which)

    bytes_of(fall.at[:, pl.ds(0, 7 * tok)], f_s.at[0]).wait()
    bytes_of(dall.at[pl.ds(0, 7 * tok)], d_s.at[0]).wait()
    for sent, sem in ((ysend, y_s), (yu_out, yu_s), (msend, m_s), (mu_out, mu_s)):
        bytes_of(sent, sem.at[0]).wait()


def sizes(row_count, cols, features, cotangent):
    lines = row_count // 2
    tokens = 2 * features.shape[0] * cols
    rows = features.shape[1] // lines
    width = cotangent.shape[1] // cols
    return lines, tokens, rows, width


def fused(row_count, cols, features, cotangent):
    lines, tokens, rows, width = sizes(row_count, cols, features, cotangent)
    chunks, half = len(WIDTHS), rows // 2
    dma = pltpu.SemaphoreType.DMA
    coded = pltpu.VMEM((2, half, width), jnp.bfloat16)
    moved = pltpu.VMEM((half, width), jnp.bfloat16)
    coded_undo = pltpu.VMEM((2, 1, width), jnp.float32)
    moved_undo = pltpu.VMEM((1, width), jnp.float32)
    return pl.pallas_call(
        functools.partial(kernel, lines, cols),
        out_shape=pltpu.VMEM((half, width), jnp.float32),
        in_specs=[pl.BlockSpec(memory_space=pl.ANY)] * 2,
        out_specs=pl.BlockSpec(memory_space=pltpu.VMEM),
        scratch_shapes=[
            pltpu.VMEM((4, tokens, half), jnp.bfloat16),
            pltpu.VMEM((tokens, width), jnp.bfloat16),
            pltpu.VMEM((half, max(WIDTHS) * width // PARTS), jnp.float32),
            coded, coded, coded_undo, coded_undo,
            pltpu.VMEM((half, width), jnp.float32),
            moved, moved, moved_undo, moved_undo,
            dma((1,)), dma((4,)), dma((4, 2)), dma((4,)),
            dma((1,)), dma((chunks, 2)), dma((chunks,)),
            dma((1,)), dma((2, chunks)), dma((1,)), dma((2, chunks)),
            dma((1,)), dma((chunks,)), dma((1,)), dma((chunks,)),
        ],
        compiler_params=pltpu.CompilerParams(
            collective_id=0, has_side_effects=True, vmem_limit_bytes=VMEM_MOST
        ),
    )(features, cotangent)


def fits(row_count, cols, features, cotangent):
    if row_count != 8 or cols != 4 or cotangent.shape[1] % (cols * PARTS * 128):
        return False
    if features.shape[1] % (row_count * 128) or features.shape[0] % 16:
        return False
    lines, tokens, rows, width = sizes(row_count, cols, features, cotangent)
    held = 2 * tokens * (2 * rows + width) + 11 * rows * width + 4 * rows * width // 8
    return held <= VMEM_MOST


def local(row_count, cols, features, cotangent):
    if fits(row_count, cols, features, cotangent):
        return fused(row_count, cols, features, cotangent)
    return plain(features, cotangent)


def solution(mesh):
    placed = (P(("row", "col"), None), P(("row", "col"), None))
    body = functools.partial(local, mesh.shape["row"], mesh.shape["col"])
    return jax.shard_map(
        body, mesh=mesh, in_specs=placed, out_specs=P("row", "col"), check_vma=False
    )
```

```python
import functools

import jax
import jax.numpy as jnp
from jax import lax
from jax.experimental import pallas as pl
from jax.experimental.pallas import tpu as pltpu
from jax.sharding import PartitionSpec as P

MESH = pl.DeviceIdType.MESH
WIDTHS = (1, 1, 1, 1, 1, 1, 1, 1)
PARTS = sum(WIDTHS)
STRIP = 64
PEAK = 250.0
VMEM_MOST = 58 * 1024 * 1024


ORDER = (
    ("Z", 0), ("Z", 2), ("F", 0), ("D", 0), ("relay", 0), ("forward", "F", 0), ("P", 0),
    ("relay_across", 0), ("D", 1), ("relay", 1), ("forward", "P", 0), ("D", 2), ("relay", 2),
    ("give", 0, 0), ("relay_across", 1), ("D", 3), ("relay", 3), ("relay_across", 2), ("D", 4),
    ("relay", 4), ("relay_across", 3), ("F", 2), ("give", 0, 1), ("relay_across", 4), ("P", 2),
    ("forward", "F", 2), ("D", 5), ("relay", 5), ("give", 0, 2), ("forward", "P", 2), ("F", 3),
    ("keep", 0, 2), ("keep", 0, 1), ("relay_across", 5), ("D", 6), ("finish", 0, 1),
    ("keep", 0, 0), ("finish", 0, 0), ("relay", 6), ("forward", "F", 3), ("F", 1),
    ("give", 0, 3), ("finish", 0, 2), ("keep", 0, 3), ("relay_across", 6), ("give", 0, 4),
    ("Z", 1), ("Z", 3), ("D", 7), ("keep", 0, 4), ("relay", 7), ("forward", "F", 1),
    ("finish", 0, 3), ("relay_across", 7), ("give", 0, 5), ("far", 0), ("far", 1), ("far", 2),
    ("far", 3), ("keep", 0, 5), ("finish", 0, 4), ("far", 4), ("give", 0, 6), ("finish", 0, 5),
    ("far", 5), ("keep", 0, 6), ("P", 1), ("P", 3), ("finish", 0, 6), ("far", 6),
    ("forward", "P", 1), ("give", 1, 6), ("forward", "P", 3), ("keep", 1, 0), ("give", 0, 7),
    ("keep", 0, 7), ("keep", 1, 5), ("keep", 1, 7), ("keep", 1, 3), ("keep", 1, 4),
    ("give", 1, 1), ("keep", 1, 2), ("keep", 1, 6), ("finish", 0, 7), ("far", 7),
    ("finish", 1, 6), ("keep", 1, 1), ("give", 1, 3), ("finish", 1, 1), ("last", 1),
    ("give", 1, 7), ("finish", 1, 3), ("give", 1, 4), ("finish", 1, 7), ("give", 1, 0),
    ("last", 3), ("finish", 1, 4), ("give", 1, 5), ("last", 4), ("finish", 1, 0), ("last", 0),
    ("give", 1, 2), ("finish", 1, 5), ("last", 5), ("last", 6), ("finish", 1, 2), ("last", 2),
    ("last", 7),
)


def tokens_product(left, right):
    return lax.dot_general(
        left, right, (((0,), (0,)), ((), ())), preferred_element_type=jnp.float32
    )


def plain(features, cotangent):
    row_count = lax.axis_size("row")
    width_in = features.shape[1]
    local_rows = width_in // row_count
    columns = lax.all_to_all(cotangent, "col", split_axis=1, concat_axis=0, tiled=True)
    tok_local = features.shape[0]
    exchanged = lax.all_to_all(features, "row", split_axis=1, concat_axis=0, tiled=True)
    stacked = exchanged.reshape(row_count, tok_local, local_rows)
    gathered = lax.all_gather(stacked, "col", axis=1, tiled=True)
    all_tokens = gathered.reshape(-1, local_rows)
    return tokens_product(all_tokens, lax.all_gather(columns, "row", axis=0, tiled=True))


def encode(src, dst, undo_row):
    rows, width = src.shape

    def strip(s):
        return pl.ds(pl.multiple_of(s * STRIP, STRIP), STRIP)

    top = lax.fori_loop(
        0, rows // STRIP, lambda s, m: jnp.maximum(m, jnp.abs(src[strip(s), :])),
        jnp.zeros((STRIP, width), jnp.float32),
    )
    undo = jnp.maximum(jnp.max(top, axis=0, keepdims=True), 4e-36) * (1.0 / PEAK)
    undo_row[...] = undo
    scale = 1.0 / undo

    @pl.loop(0, rows // STRIP)
    def _(s):
        t = src[strip(s), :] * scale
        u = t * t
        u = u * u
        u = u * u
        u = u * u
        dst[strip(s), :] = jnp.where(t < 0, -u, u).astype(jnp.bfloat16)


def decode_add(src, undo_row, into):
    undo = undo_row[...]

    @pl.loop(0, into.shape[0] // STRIP)
    def _(s):
        span = pl.ds(pl.multiple_of(s * STRIP, STRIP), STRIP)
        b = src[span, :].astype(jnp.float32)
        root = lax.rsqrt(jnp.maximum(jnp.abs(b), 1e-37))
        most = lax.rsqrt(lax.rsqrt(lax.rsqrt(root)))
        into[span, :] += (b * root) * root * most * undo


def kernel(
    lines, cols, feat, cot, out,
    fall, dall, tmp, ysend, yrecv, yu_out, yu_in, acc, msend, mrecv, mu_out, mu_in,
    f_s, fz_r, fx_r, fm_r, d_s, dx_r, dz_r, y_s, y_r, yu_s, yu_r, m_s, m_r, mu_s, mu_r,
):
    row = lax.axis_index("row")
    col = lax.axis_index("col")
    z, y = row // 2, row % 2
    here = z % 2
    near = z + 1 - 2 * here
    far = lines - 1 - z
    inner = (z > 0) & (z < lines - 1)
    tok = feat.shape[0]
    half = fall.shape[2]
    chunks = len(WIDTHS)
    width = dall.shape[1]
    part = width // PARTS

    def cols_of(j):
        return pl.ds(sum(WIDTHS[:j]) * part, WIDTHS[j] * part)


    def at_row(zz, yy):
        return {"row": zz * 2 + yy, "col": col}

    pair, mirror, partner = at_row(near, y), at_row(far, y), at_row(z, 1 - y)
    mate_col = col + 1 - 2 * (col % 2)
    col_of = (col, mate_col, (col + 2) % cols, (mate_col + 2) % cols)
    MATE, ACROSS = 1, 2

    def at_col(k):
        return {"row": row, "col": col_of[k]}

    def remote(src, dst, s, r, dev):
        return pltpu.make_async_remote_copy(
            src_ref=src, dst_ref=dst, send_sem=s, recv_sem=r,
            device_id=dev, device_id_type=MESH,
        )

    barrier = pltpu.get_barrier_semaphore()
    others = [pair, mirror, partner] + [at_col(k) for k in range(1, cols)]
    for dev in others:
        pl.semaphore_signal(barrier, inc=1, device_id=dev, device_id_type=MESH)
    pl.semaphore_wait(barrier, len(others))

    def slot(plane, c):
        return pl.ds(pl.multiple_of((plane * cols + c) * tok, tok), tok)

    def f_cols(zz, q):
        wanted = lines - 1 - zz if q % 2 == 0 else zz
        yy = 1 - y if q < 2 else y
        return feat.at[:, pl.ds(pl.multiple_of((wanted * 2 + yy) * half, half), half)]

    def f_own(q):
        return pltpu.make_async_copy(f_cols(z, q), fall.at[q, slot(here, col)], fm_r.at[q])

    def f_pair(q):
        return remote(f_cols(near, q), fall.at[q, slot(here, col)], f_s.at[0], fz_r.at[q], pair)

    def f_block(q, other, k):
        return fall.at[q, slot(1 - here if other else here, col_of[k])]

    def f_across(q, other):
        block = f_block(q, other, 0)
        src = block if other else f_cols(z, q)
        return remote(src, block, f_s.at[0], fx_r.at[q, other], at_col(ACROSS))

    def f_mate(q, other, k):
        block = f_block(q, other, ACROSS * k)
        src = f_cols(z, q) if not other and not k else block
        return remote(src, block, f_s.at[0], fm_r.at[q], at_col(MATE))

    def d_cols(cc, j):
        first = pl.multiple_of(cc * width + sum(WIDTHS[:j]) * part, part)
        return cot.at[:, pl.ds(first, WIDTHS[j] * part)]

    def d_own(j):
        return pltpu.make_async_copy(d_cols(col, j), dall.at[slot(here, col), cols_of(j)], dz_r.at[j])

    def d_send(j, k):
        return remote(
            d_cols(col_of[k], j), dall.at[slot(here, col), cols_of(j)],
            d_s.at[0], dx_r.at[j, k // ACROSS], at_col(k),
        )

    def d_block(j, k):
        if k < ACROSS:
            return dall.at[slot(here, col_of[k]), cols_of(j)]
        first = (here * cols + (col // 2 * 2 + 2) % cols) * tok
        return dall.at[pl.ds(pl.multiple_of(first, tok), 2 * tok), cols_of(j)]

    def d_recv(j, k):
        block = d_block(j, k)
        return remote(block, block, d_s.at[0], dx_r.at[j, k // ACROSS], at_col(k))

    def d_pair(j, k):
        block = d_block(j, k)
        return remote(block if k else d_cols(col, j), block, d_s.at[0], dz_r.at[j], pair)

    def bytes_of(block, sem):
        return pltpu.make_async_copy(block, block, sem)

    def y_copies(g, j):
        c = cols_of(j)
        return (
            remote(yu_out.at[g, :, c], yu_in.at[g, :, c], yu_s.at[0], yu_r.at[g, j], partner),
            remote(ysend.at[g, :, c], yrecv.at[g, :, c], y_s.at[0], y_r.at[g, j], partner),
        )

    def m_copies(j):
        c = cols_of(j)
        return (
            remote(mu_out.at[:, c], mu_in.at[:, c], mu_s.at[0], mu_r.at[j], mirror),
            remote(msend.at[:, c], mrecv.at[:, c], m_s.at[0], m_r.at[j], mirror),
        )

    def start(copies):
        for copy in copies:
            copy.start()

    def receive(copies):
        for copy in copies:
            copy.wait_recv()

    def total(g, j):
        return (out if g else acc).at[:, cols_of(j)]

    ready = set()

    def once(key):
        new = key not in ready
        ready.add(key)
        return new

    def arrive(q, j):
        if once(("F", q)):
            bytes_of(fall.at[q, pl.ds(0, 5 * tok)], fm_r.at[q]).wait()
        if once(("D", j)):
            bytes_of(dall.at[pl.ds(0, 5 * tok), cols_of(j)], dz_r.at[j]).wait()

    def do_Z(q):
        f_pair(q).start()

    def do_F(q):
        f_across(q, 0).start()
        f_mate(q, 0, 0).start()
        f_own(q).start()

    def do_P(q):
        f_pair(q).wait_recv()
        f_across(q, 1).start()
        f_mate(q, 1, 0).start()

    def do_D(j):
        d_pair(j, 0).start()
        for k in (2, 3, 1):
            d_send(j, k).start()
        d_own(j).start()

    def do_forward(kind, q):
        other = 1 if kind == "P" else 0
        f_across(q, other).wait_recv()
        f_mate(q, other, 1).start()

    def do_relay(j):
        d_recv(j, MATE).wait_recv()
        d_pair(j, MATE).start()

    def do_relay_across(j):
        d_recv(j, ACROSS).wait_recv()
        d_pair(j, ACROSS).start()

    def do_give(g, j):
        arrive(g, j)
        c = cols_of(j)
        made = tmp.at[:, pl.ds(0, c.size)]
        made[...] = tokens_product(fall[g], dall[:, c])
        encode(made, ysend.at[g, :, c], yu_out.at[g, :, c])
        start(y_copies(g, j))

    def do_keep(g, j):
        arrive(2 + g, j)
        total(g, j)[...] = tokens_product(fall[2 + g], dall[:, cols_of(j)])

    def do_finish(g, j):
        receive(y_copies(g, j))
        c = cols_of(j)
        decode_add(yrecv.at[g, :, c], yu_in.at[g, :, c], total(g, j))
        if g == 0:
            encode(total(0, j), msend.at[:, c], mu_out.at[:, c])

            @pl.when(inner)
            def _():
                start(m_copies(j))

    def do_far(j):
        @pl.when(~inner)
        def _():
            start(m_copies(j))

    def do_last(j):
        receive(m_copies(j))
        c = cols_of(j)
        decode_add(mrecv.at[:, c], mu_in.at[:, c], total(1, j))

    run = {
        "Z": do_Z, "F": do_F, "P": do_P, "far": do_far, "D": do_D, "forward": do_forward, "relay": do_relay,
        "relay_across": do_relay_across, "give": do_give, "keep": do_keep,
        "finish": do_finish, "last": do_last,
    }
    for name, *which in ORDER:
        with jax.named_scope(name + "".join(str(w) for w in which)):
            run[name](*which)

    bytes_of(fall.at[:, pl.ds(0, 7 * tok)], f_s.at[0]).wait()
    bytes_of(dall.at[pl.ds(0, 7 * tok)], d_s.at[0]).wait()
    for sent, sem in ((ysend, y_s), (yu_out, yu_s), (msend, m_s), (mu_out, mu_s)):
        bytes_of(sent, sem.at[0]).wait()


def sizes(row_count, cols, features, cotangent):
    lines = row_count // 2
    tokens = 2 * features.shape[0] * cols
    rows = features.shape[1] // lines
    width = cotangent.shape[1] // cols
    return lines, tokens, rows, width


def fused(row_count, cols, features, cotangent):
    lines, tokens, rows, width = sizes(row_count, cols, features, cotangent)
    chunks, half = len(WIDTHS), rows // 2
    dma = pltpu.SemaphoreType.DMA
    coded = pltpu.VMEM((2, half, width), jnp.bfloat16)
    moved = pltpu.VMEM((half, width), jnp.bfloat16)
    coded_undo = pltpu.VMEM((2, 1, width), jnp.float32)
    moved_undo = pltpu.VMEM((1, width), jnp.float32)
    return pl.pallas_call(
        functools.partial(kernel, lines, cols),
        out_shape=pltpu.VMEM((half, width), jnp.float32),
        in_specs=[pl.BlockSpec(memory_space=pl.ANY)] * 2,
        out_specs=pl.BlockSpec(memory_space=pltpu.VMEM),
        scratch_shapes=[
            pltpu.VMEM((4, tokens, half), jnp.bfloat16),
            pltpu.VMEM((tokens, width), jnp.bfloat16),
            pltpu.VMEM((half, max(WIDTHS) * width // PARTS), jnp.float32),
            coded, coded, coded_undo, coded_undo,
            pltpu.VMEM((half, width), jnp.float32),
            moved, moved, moved_undo, moved_undo,
            dma((1,)), dma((4,)), dma((4, 2)), dma((4,)),
            dma((1,)), dma((chunks, 2)), dma((chunks,)),
            dma((1,)), dma((2, chunks)), dma((1,)), dma((2, chunks)),
            dma((1,)), dma((chunks,)), dma((1,)), dma((chunks,)),
        ],
        compiler_params=pltpu.CompilerParams(
            collective_id=0, has_side_effects=True, vmem_limit_bytes=VMEM_MOST
        ),
    )(features, cotangent)


def fits(row_count, cols, features, cotangent):
    if row_count != 8 or cols != 4 or cotangent.shape[1] % (cols * PARTS * 128):
        return False
    if features.shape[1] % (row_count * 128) or features.shape[0] % 16:
        return False
    lines, tokens, rows, width = sizes(row_count, cols, features, cotangent)
    held = 2 * tokens * (2 * rows + width) + 11 * rows * width + 4 * rows * width // 8
    return held <= VMEM_MOST


def local(row_count, cols, features, cotangent):
    if fits(row_count, cols, features, cotangent):
        return fused(row_count, cols, features, cotangent)
    return plain(features, cotangent)


def solution(mesh):
    placed = (P(("row", "col"), None), P(("row", "col"), None))
    body = functools.partial(local, mesh.shape["row"], mesh.shape["col"])
    return jax.shard_map(
        body, mesh=mesh, in_specs=placed, out_specs=P("row", "col"), check_vma=False
    )
```
